32 devices in a mesh: groups: 2 (over x), blk: 16 (over z, y, core).
Axes of the slice: x: 2, y: 2, z: 4, core: 2. Of those that a mesh axis runs over, the one named last changes fastest.
Arguments:
- queries: bfloat16 [4096, 4096], P(('groups', 'blk')), parts along dimension 0, may hold values from -96 to 96
- keys: bfloat16 [4096, 512], P(('groups', 'blk')), parts along dimension 0, may hold values from -3 to 3
- values: bfloat16 [4096, 512], P(('groups', 'blk')), parts along dimension 0, may hold values from -4 to 4
- out_packed: int32 [4096, 512], P('blk'), may hold values from -2147483648 to 2147483646
- out_scales: bfloat16 [32, 4096], replicated, may hold values from 0.0029907227 to 0.029907227
- hadamard_signs: int32 [4096], replicated, may hold values from 0 to 1
Outputs:
- mixed: bfloat16 [4096, 4096], P(('groups', 'blk')), parts along dimension 0
The draws below stay inside these ranges and needn't reach their ends.
There are 2 independent parts, one for each index of `groups`. The reference program is written for one: setup_inputs(seed, part) draws one part's arguments, and reference() takes and returns one part's arrays. A program takes and returns all parts, laid end to end along the dimension named above; an argument that names none is the same for every part. Nothing has to cross between parts.
All inputs are finite; a program needn't handle non-finite values.
Results may differ from the reference program's by a relative error of at most 0.012.
Values may be sent and summed in bfloat16 or wider, within the bound.
A program may use at most 256 MiB of HBM per device.

```python
import math
import jax
import jax.numpy as jnp
from jax import lax

HEAD_SIZE = 128
QUERY_HEADS = 32
KEY_VALUE_HEADS = 4
DO = 4096
GROUP = 128
SEQUENCE_LENGTH = 2048


def make_pair(key):
    base = jax.random.fold_in(key, 31)
    key_query, key_keys = jax.random.split(base, 2)
    query_width = QUERY_HEADS * HEAD_SIZE
    keys_width = KEY_VALUE_HEADS * HEAD_SIZE
    query_table = 2.5 * jax.random.truncated_normal(key_query, -3.0, 3.0, (SEQUENCE_LENGTH, query_width), jnp.float32)
    key_rows_table = jax.random.truncated_normal(key_keys, -3.0, 3.0, (SEQUENCE_LENGTH, keys_width), jnp.float32)
    return (query_table, key_rows_table)


def draw_queries(key, part):
    return make_pair(key)[0].astype(jnp.bfloat16)


def draw_keys(key, part):
    return make_pair(key)[1].astype(jnp.bfloat16)


def with_ends(values, rng, smallest, top_value):
    longest = values.shape.index(max(values.shape))
    spots = []
    for shift in (0, 1):
        where = [jax.random.randint(jax.random.fold_in(rng, axis), (), 0, length) for axis, length in enumerate(values.shape)]
        where[longest] = (where[longest] + shift) % values.shape[longest]
        spots.append(tuple(where))
    return values.at[spots[0]].set(smallest).at[spots[1]].set(top_value)


def steps_of(own_key, extent, cuts, smallest, high):
    factor_of = 1.0
    for axis_at, blocks in cuts:
        draws = jax.random.uniform(jax.random.fold_in(jax.random.fold_in(own_key, 6), axis_at), (blocks,), jnp.float32, smallest / len(cuts), high / len(cuts))
        factor_of = factor_of * jnp.repeat(jnp.exp(draws), extent[axis_at] // blocks).reshape((-1,) + (1,) * (len(extent) - 1 - axis_at))
    return factor_of


def noise(stream_key, dims, spread, bound, pieces=(), kind=jnp.bfloat16):
    values = jax.random.normal(stream_key, dims, jnp.float32) * spread
    if len(pieces) > 0:
        values = steps_of(stream_key, dims, pieces, -0.22, 0.18) * values
    return jnp.clip(values, min=-bound, max=bound).astype(kind)


def setup_inputs(seed: int = 0, part: int = 0) -> dict:
    splits = jax.random.split(jax.random.key(seed), 7)
    own_keys = jax.random.split(jax.random.fold_in(splits[6], part), 7)
    queries = draw_queries(jax.random.fold_in(jax.random.fold_in(splits[6], part), 71), part)
    keys = draw_keys(jax.random.fold_in(jax.random.fold_in(splits[6], part), 71), part)
    values = noise(own_keys[2], (SEQUENCE_LENGTH, KEY_VALUE_HEADS * HEAD_SIZE), 1.0, 4.0, ((0, 16),))
    out_packed = with_ends(jax.random.randint(splits[3], (QUERY_HEADS * HEAD_SIZE, DO // 8), -2147483648, 2147483647), jax.random.fold_in(splits[3], 1), -2147483648, 2147483646).astype(jnp.int32)
    out_scales = jnp.clip(jnp.exp(jax.random.uniform(splits[4], (QUERY_HEADS * HEAD_SIZE // GROUP, DO), jnp.float32, math.log(0.0029907227), math.log(0.029907227))), 0.0029907227, 0.029907227).astype(jnp.bfloat16)
    hadamard_signs = with_ends(jax.random.randint(splits[5], (QUERY_HEADS * HEAD_SIZE,), 0, 2), jax.random.fold_in(splits[5], 1), 0, 1).astype(jnp.int32)
    return {"queries": queries, "keys": keys, "values": values, "out_packed": out_packed, "out_scales": out_scales, "hadamard_signs": hadamard_signs}


def sylvester(block_count):
    index = jnp.arange(block_count, dtype=jnp.int32)
    both = jnp.bitwise_and(index[:, None], index[None, :])
    parity = jnp.zeros((block_count, block_count), jnp.int32)
    for bit_number in range(block_count.bit_length() - 1):
        parity = jnp.bitwise_xor(parity, jnp.bitwise_and(jnp.right_shift(both, bit_number), 1))
    return (1 - 2 * parity).astype(jnp.float32)

def rotate(attention, hadamard_signs):
    block_count = attention.shape[0]
    signed = attention.astype(jnp.float32) * (2 * hadamard_signs - 1).astype(jnp.float32)
    inner = jnp.einsum('rhd,de->rhe', signed.reshape(block_count, QUERY_HEADS, HEAD_SIZE), sylvester(HEAD_SIZE), precision=lax.Precision.HIGHEST)
    outer = jnp.einsum('gh,rhe->rge', sylvester(QUERY_HEADS), inner, precision=lax.Precision.HIGHEST)
    return (outer * (1.0 / math.sqrt(QUERY_HEADS * HEAD_SIZE))).reshape(block_count, QUERY_HEADS * HEAD_SIZE).astype(jnp.bfloat16)

def dequantize(packed, scale_rows):
    fields = [jnp.bitwise_and(jnp.right_shift(packed, 4 * nibble), 15) for nibble in range(8)]
    levels = jnp.concatenate(fields, axis=1) - 8
    return (levels.astype(jnp.float32) * scale_rows.astype(jnp.float32)).astype(jnp.bfloat16)

def reference(queries, keys, values, out_packed, out_scales, hadamard_signs):
    head_group = QUERY_HEADS // KEY_VALUE_HEADS
    block_number = math.gcd(SEQUENCE_LENGTH, 128)
    scale = 1.0 / math.sqrt(HEAD_SIZE)
    gathered_keys = keys.astype(jnp.float32).reshape(SEQUENCE_LENGTH, KEY_VALUE_HEADS, HEAD_SIZE)
    gathered_values = values.astype(jnp.float32).reshape(SEQUENCE_LENGTH, KEY_VALUE_HEADS, HEAD_SIZE)
    key_positions = jnp.arange(SEQUENCE_LENGTH, dtype=jnp.int32)

    def attend(start_offset):
        query_tile = lax.dynamic_slice_in_dim(queries, start_offset, block_number, 0).astype(jnp.float32).reshape(block_number, KEY_VALUE_HEADS, head_group, HEAD_SIZE)
        scores = jnp.einsum('qkgd,nkd->kgqn', query_tile, gathered_keys, precision=lax.Precision.HIGHEST) * scale
        query_positions = start_offset + jnp.arange(block_number, dtype=jnp.int32)
        allowed = query_positions[:, None] >= key_positions[None, :]
        scores = jnp.where(allowed, scores, -jnp.inf)
        largest = lax.optimization_barrier(jnp.max(scores, axis=-1, keepdims=True))
        weights = jnp.exp(scores - largest)
        totals = lax.optimization_barrier(jnp.sum(weights, axis=-1))
        rounded = lax.optimization_barrier(weights.astype(jnp.bfloat16)).astype(jnp.float32)
        summed = jnp.einsum('kgqn,nkd->qkgd', rounded, gathered_values, precision=lax.Precision.HIGHEST)
        summed = summed / jnp.transpose(totals, (2, 0, 1))[..., None]
        return summed.reshape(block_number, QUERY_HEADS * HEAD_SIZE).astype(jnp.bfloat16)
    starts = jnp.arange(SEQUENCE_LENGTH // block_number, dtype=jnp.int32) * block_number
    attention = lax.map(attend, starts).reshape(SEQUENCE_LENGTH, QUERY_HEADS * HEAD_SIZE)
    rotated = rotate(attention, hadamard_signs)
    scale_rows = jnp.repeat(out_scales, GROUP, axis=0)
    weight = dequantize(out_packed, scale_rows)
    return jnp.dot(rotated, weight, preferred_element_type=jnp.float32).astype(jnp.bfloat16)
```

```python
import functools
import math

import jax
import jax.numpy as jnp
from jax import lax
from jax.experimental import pallas as pl
from jax.experimental.pallas import tpu as pltpu
from jax.sharding import PartitionSpec as P

HEAD_SIZE = 128
QUERY_HEADS = 32
KEY_VALUE_HEADS = 4
GROUP = 128
HEAD_GROUP = QUERY_HEADS // KEY_VALUE_HEADS
NEGATIVE = -1e30
EXPONENT = math.log2(math.e) / math.sqrt(HEAD_SIZE)
MESH = pl.DeviceIdType.MESH


def sylvester(block_count):
    index = jnp.arange(block_count, dtype=jnp.int32)
    both = jnp.bitwise_and(index[:, None], index[None, :])
    parity = jnp.zeros((block_count, block_count), jnp.int32)
    for bit_number in range(block_count.bit_length() - 1):
        parity = jnp.bitwise_xor(parity, jnp.bitwise_and(jnp.right_shift(both, bit_number), 1))
    return (1 - 2 * parity).astype(jnp.bfloat16)


def kernel(
    n, groups, share, early,
    q_ref, kv_ref, packed_ref, scales_ref, signs_ref, table_ref, out_ref,
    kv_all, packed_all, qs, acc, largest, totals, inner, rotated, weight,
    local_sem, kv_send, kv_recv, kv_psend, kv_precv, p_send, p_recv, p_psend, p_precv,
    x_send, x_recv, x_psend, x_precv,
):
    rows = q_ref.shape[0]
    half_rows = rows // 2
    packed_rows = packed_ref.shape[0]
    words = packed_ref.shape[1]
    share_rows = packed_rows // share
    seg = share_rows // 2
    chips = n // 2
    kv_width = KEY_VALUE_HEADS * HEAD_SIZE

    me = lax.axis_index("blk")
    my_group = lax.axis_index("groups")
    core = lax.rem(me, 2)
    partner = me + 1 - 2 * core
    chip = me // 2
    pos = jnp.where(lax.rem(chip, 2) == 0, chip // 2, chips - 1 - chip // 2)

    def chip_at(place):
        place = lax.rem(place + chips, chips)
        return jnp.where(place < chips // 2, 2 * place, 2 * (chips - 1 - place) + 1)

    after = chip_at(pos + 1) * 2 + core
    before = chip_at(pos - 1) * 2 + core
    ring_to = (after, before)
    my_share = my_group if share > 1 else jnp.int32(0)

    barrier = pltpu.get_barrier_semaphore()
    for target in (after, before, partner):
        pl.semaphore_signal(barrier, inc=1, device_id={"blk": target}, device_id_type=MESH)
    for j in range(1, share):
        pl.semaphore_signal(
            barrier, inc=1, device_id={"groups": lax.rem(my_group + j, groups)}, device_id_type=MESH
        )
    pl.semaphore_wait(barrier, 3 + share - 1)

    def owner_chip(d, s):
        return chip_at(pos - s) if d == 0 else chip_at(pos + s)

    def kv_rows(owner, d):
        return pl.ds(pl.multiple_of(owner * rows + d * half_rows, half_rows), half_rows)

    def p_rows(owner, piece, d):
        return pl.ds(
            pl.multiple_of(owner * packed_rows + piece * share_rows + d * seg, seg), seg
        )

    def remote(src, dst, send, recv, device):
        return pltpu.make_async_remote_copy(
            src_ref=src, dst_ref=dst, send_sem=send, recv_sem=recv,
            device_id=device, device_id_type=MESH,
        )

    def kv_ring(d, s):
        where = kv_all.at[kv_rows(owner_chip(d, s) * 2 + core, d)]
        return remote(where, where, kv_send.at[d, s], kv_recv.at[d, s + 1], {"blk": ring_to[d]})

    def kv_relay(d, s):
        where = kv_all.at[kv_rows(owner_chip(d, s) * 2 + core, d)]
        return remote(where, where, kv_psend.at[d, s], kv_precv.at[d, s], {"blk": partner})

    def p_ring(d, s):
        where = packed_all.at[p_rows(owner_chip(d, s) * 2 + core, my_share, d)]
        return remote(where, where, p_send.at[d, s], p_recv.at[d, s + 1], {"blk": ring_to[d]})

    def p_relay(d, s):
        where = packed_all.at[p_rows(owner_chip(d, s) * 2 + core, my_share, d)]
        return remote(where, where, p_psend.at[d, s], p_precv.at[d, s], {"blk": partner})

    def x_copy(j, d, s):
        where = packed_all.at[p_rows(owner_chip(d, s) * 2 + core, my_share, d)]
        return remote(
            where, where, x_send.at[j - 1, d, s], x_recv.at[j - 1, d, s],
            {"groups": lax.rem(my_group + j, groups)},
        )

    def x_relay(j, d, s):
        piece = lax.rem(my_group - j + groups, groups)
        where = packed_all.at[p_rows(owner_chip(d, s) * 2 + core, piece, d)]
        return remote(
            where, where, x_psend.at[j - 1, d, s], x_precv.at[j - 1, d, s], {"blk": partner}
        )

    own_kv = kv_all.at[pl.ds(pl.multiple_of(me * rows, rows), rows)]
    own_packed = packed_all.at[pl.ds(pl.multiple_of(me * packed_rows, packed_rows), packed_rows)]
    kv_local = pltpu.make_async_copy(kv_ref, own_kv, local_sem.at[0])
    p_local = pltpu.make_async_copy(packed_ref, own_packed, local_sem.at[1])
    kv_own = remote(kv_ref, own_kv, kv_psend.at[0, 0], kv_precv.at[0, 0], {"blk": partner})
    p_own = remote(packed_ref, own_packed, p_psend.at[0, 0], p_precv.at[0, 0], {"blk": partner})
    kv_local.start()
    p_local.start()
    kv_local.wait()
    kv_own.start()
    for d in (0, 1):
        kv_ring(d, 0).start()
    p_local.wait()
    for d in (0, 1):
        p_ring(d, 0).start()
    p_own.start()

    for h in range(QUERY_HEADS):
        g, r = divmod(h, HEAD_GROUP)
        qs[g, r * rows:(r + 1) * rows, :] = q_ref[:, h * HEAD_SIZE:(h + 1) * HEAD_SIZE]

    def attend(pieces, bias, first):
        tile = 2 * rows
        for g in range(KEY_VALUE_HEADS):
            k = jnp.concatenate(
                [kv_all[p, g * HEAD_SIZE:(g + 1) * HEAD_SIZE] for p in pieces], axis=0
            )
            v = jnp.concatenate(
                [kv_all[p, kv_width + g * HEAD_SIZE:kv_width + (g + 1) * HEAD_SIZE] for p in pieces],
                axis=0,
            )
            vt = v.T
            for c in range(HEAD_GROUP * rows // tile):
                cols = slice(c * tile, (c + 1) * tile)
                scores = lax.dot_general(
                    k, qs[g, cols, :], (((1,), (1,)), ((), ())), preferred_element_type=jnp.float32
                )
                scores = scores + bias
                top = jnp.max(scores, axis=0, keepdims=True)
                if not first:
                    old = largest[g, :, cols]
                    top = jnp.maximum(old, top)
                    fading = jnp.exp2((old - top) * EXPONENT)
                weights = jnp.exp2((scores - top) * EXPONENT)
                total = jnp.sum(weights, axis=0, keepdims=True)
                product = jnp.dot(
                    vt, weights.astype(jnp.bfloat16), preferred_element_type=jnp.float32
                )
                if first:
                    totals[g, :, cols] = total
                    acc[g, :, cols] = product
                else:
                    totals[g, :, cols] = totals[g, :, cols] * fading + total
                    acc[g, :, cols] = acc[g, :, cols] * fading + product
                largest[g, :, cols] = top

    chunk = math.gcd(seg, 32)

    def dequantize(row, target):
        base = packed_all[pl.ds(pl.multiple_of(row, chunk), chunk), :]
        flipped = jnp.bitwise_xor(base, jnp.int32(-2004318072))
        scale_index = row // GROUP
        for nibble in range(8):
            level = jnp.right_shift(jnp.left_shift(flipped, 28 - 4 * nibble), 28)
            scale = scales_ref[pl.ds(scale_index, 1), nibble * words:(nibble + 1) * words]
            weight[pl.ds(pl.multiple_of(target, chunk), chunk), nibble * words:(nibble + 1) * words] = (
                level.astype(jnp.float32) * scale
            ).astype(jnp.bfloat16)

    def dequantize_rows(first_row, count):
        @pl.loop(0, count // chunk)
        def _(t):
            dequantize(first_row + t * chunk, first_row + t * chunk)

    kv_own.wait_recv()
    key_pos = chip * 2 * rows + lax.broadcasted_iota(jnp.int32, (2 * rows, 2 * rows), 0)
    query_pos = me * rows + lax.rem(lax.broadcasted_iota(jnp.int32, (2 * rows, 2 * rows), 1), rows)
    attend(
        [pl.ds(pl.multiple_of(chip * 2 * rows, 2 * rows), 2 * rows)],
        jnp.where(key_pos <= query_pos, 0.0, NEGATIVE),
        True,
    )
    p_own.wait_recv()
    if early:
        dequantize_rows(chip * 2 * packed_rows, 2 * packed_rows)

    def finish_packed(s):
        for d in (0, 1):
            for j in range(1, share):
                x_copy(j, d, s).wait_recv()
                x_relay(j, d, s).start()
        for d in (0, 1):
            p_relay(d, s).wait_recv()
        def pieces(t):
            owner_core = lax.rem(t, 2)
            piece = t // 2
            for d in (0, 1):
                owner = owner_chip(d, s) * 2 + owner_core
                dequantize_rows(owner * packed_rows + piece * share_rows + d * seg, seg)
        for d in (0, 1):
            for j in range(1, share):
                x_relay(j, d, s).wait_recv()
        if early:
            pl.loop(0, 2 * share)(pieces)

    @pl.loop(1, chips)
    def _(s):
        for d in (0, 1):
            kv_ring(d, s - 1).wait_recv()

            @pl.when(s < chips - 1)
            def _():
                kv_ring(d, s).start()

            kv_relay(d, s).start()
        for d in (0, 1):
            p_ring(d, s - 1).wait_recv()

            @pl.when(s < chips - 1)
            def _():
                p_ring(d, s).start()

            for j in range(1, share):
                x_copy(j, d, s).start()
            p_relay(d, s).start()
        for d in (0, 1):
            kv_relay(d, s).wait_recv()
        first_chip, second_chip = owner_chip(0, s), owner_chip(1, s)

        @pl.when((first_chip < chip) | (second_chip < chip))
        def _():
            key_row = lax.broadcasted_iota(jnp.int32, (2 * rows, 1), 0)
            needed = jnp.where(key_row < rows, (first_chip < chip).astype(jnp.int32), (second_chip < chip).astype(jnp.int32))
            bias = jnp.where(needed > 0, 0.0, NEGATIVE)
            attend(
                [
                    kv_rows(first_chip * 2, 0), kv_rows(first_chip * 2 + 1, 0),
                    kv_rows(second_chip * 2, 1), kv_rows(second_chip * 2 + 1, 1),
                ],
                bias, False,
            )

        @pl.when(s > 1)
        def _():
            finish_packed(s - 1)

    for g in range(KEY_VALUE_HEADS):
        for r in range(HEAD_GROUP):
            h = g * HEAD_GROUP + r
            cols = slice(r * rows, (r + 1) * rows)
            attention = (acc[g, :, cols] / totals[g, :, cols]).T.astype(jnp.bfloat16)
            signed = attention * signs_ref[:, h * HEAD_SIZE:(h + 1) * HEAD_SIZE]
            inner[h] = jnp.dot(signed, table_ref[...], preferred_element_type=jnp.float32)

    @pl.loop(0, rows // 16)
    def _(t):
        these = pl.ds(pl.multiple_of(t * 16, 16), 16)
        heads = [inner[h, these, :] for h in range(QUERY_HEADS)]
        step = 1
        while step < QUERY_HEADS:
            done = list(heads)
            for h in range(QUERY_HEADS):
                if h & step == 0:
                    done[h] = heads[h] + heads[h + step]
                    done[h + step] = heads[h] - heads[h + step]
            heads = done
            step *= 2
        for h in range(QUERY_HEADS):
            rotated[these, h * HEAD_SIZE:(h + 1) * HEAD_SIZE] = (
                heads[h] * (1.0 / math.sqrt(QUERY_HEADS * HEAD_SIZE))
            ).astype(jnp.bfloat16)

    finish_packed(chips - 1)

    depth = n * packed_rows
    out_width = out_ref.shape[1]
    if early:
        tile = 512

        @pl.loop(0, out_width // tile)
        def _(t):
            cols = pl.ds(pl.multiple_of(t * tile, tile), tile)
            out_ref[:, cols] = jnp.dot(
                rotated[...], weight[:, cols], preferred_element_type=jnp.float32
            ).astype(jnp.bfloat16)
    else:
        span = weight.shape[0]
        tile = HEAD_GROUP * rows
        acc[...] = jnp.zeros_like(acc)

        @pl.loop(0, depth // span)
        def _(k):
            @pl.loop(0, span // chunk)
            def _(t):
                dequantize(k * span + t * chunk, t * chunk)

            left = rotated[:, pl.ds(pl.multiple_of(k * span, span), span)]
            for c in range(KEY_VALUE_HEADS):
                acc[c] += jnp.dot(
                    left, weight[:, c * tile:(c + 1) * tile], preferred_element_type=jnp.float32
                )

        for c in range(KEY_VALUE_HEADS):
            out_ref[:, c * tile:(c + 1) * tile] = acc[c].astype(jnp.bfloat16)

    kv_own.wait_send()
    p_own.wait_send()
    for d in (0, 1):
        kv_ring(d, 0).wait_send()
        p_ring(d, 0).wait_send()

    @pl.loop(1, chips)
    def _(s):
        for d in (0, 1):
            @pl.when(s < chips - 1)
            def _():
                kv_ring(d, s).wait_send()
                p_ring(d, s).wait_send()

            kv_relay(d, s).wait_send()
            p_relay(d, s).wait_send()
            for j in range(1, share):
                x_copy(j, d, s).wait_send()
                x_relay(j, d, s).wait_send()


def local(n, groups, queries, keys, values, out_packed, out_scales, hadamard_signs):
    rows = queries.shape[0]
    packed_rows, words = out_packed.shape
    width = queries.shape[1]
    share = groups if packed_rows % (32 * groups) == 0 else 1
    chips = n // 2
    kv = jnp.concatenate([keys, values], axis=1)
    scales = out_scales.astype(jnp.float32)
    signs = (2 * hadamard_signs - 1).astype(jnp.bfloat16).reshape(1, width)
    depth = n * packed_rows
    out_width = 8 * words
    kv_bytes = n * rows * kv.shape[1] * 2
    early = kv_bytes + depth * out_width * 2 + depth * words * 4 < 46 * 2**20
    others = max(share - 1, 1)
    dma = pltpu.SemaphoreType.DMA
    spec = pl.BlockSpec(memory_space=pltpu.VMEM)
    return pl.pallas_call(
        functools.partial(kernel, n, groups, share, early),
        out_shape=jax.ShapeDtypeStruct((rows, out_width), jnp.bfloat16),
        in_specs=[spec] * 6,
        out_specs=spec,
        scratch_shapes=[
            pltpu.VMEM((n * rows, kv.shape[1]), jnp.bfloat16),
            pltpu.VMEM((depth, words), jnp.int32),
            pltpu.VMEM((KEY_VALUE_HEADS, HEAD_GROUP * rows, HEAD_SIZE), jnp.bfloat16),
            pltpu.VMEM((KEY_VALUE_HEADS, HEAD_SIZE, HEAD_GROUP * rows), jnp.float32),
            pltpu.VMEM((KEY_VALUE_HEADS, 1, HEAD_GROUP * rows), jnp.float32),
            pltpu.VMEM((KEY_VALUE_HEADS, 1, HEAD_GROUP * rows), jnp.float32),
            pltpu.VMEM((QUERY_HEADS, rows, HEAD_SIZE), jnp.float32),
            pltpu.VMEM((rows, width), jnp.bfloat16),
            pltpu.VMEM((depth if early else 256, out_width), jnp.bfloat16),
            dma((2,)),
        ]
        + [dma((2, chips))] * 8
        + [dma((others, 2, chips))] * 4,
        compiler_params=pltpu.CompilerParams(
            collective_id=0, has_side_effects=True, vmem_limit_bytes=64000000
        ),
    )(queries, kv, out_packed, scales, signs, sylvester(HEAD_SIZE))


def solution(mesh):
    in_specs = (
        P(("groups", "blk"), None),
        P(("groups", "blk"), None),
        P(("groups", "blk"), None),
        P("blk", None),
        P(),
        P(),
    )
    out_specs = P(("groups", "blk"), None)
    body = functools.partial(local, mesh.shape["blk"], mesh.shape["groups"])
    return jax.shard_map(body, mesh=mesh, in_specs=in_specs, out_specs=out_specs, check_vma=False)
```

```python
import functools
import math

import jax
import jax.numpy as jnp
from jax import lax
from jax.experimental import pallas as pl
from jax.experimental.pallas import tpu as pltpu
from jax.sharding import PartitionSpec as P

HEAD_SIZE = 128
QUERY_HEADS = 32
KEY_VALUE_HEADS = 4
GROUP = 128
HEAD_GROUP = QUERY_HEADS // KEY_VALUE_HEADS
NEGATIVE = -1e30
EXPONENT = math.log2(math.e) / math.sqrt(HEAD_SIZE)
MESH = pl.DeviceIdType.MESH


def kernel(
    n, groups, share, early,
    q_ref, k_ref, v_ref, packed_ref, scales_ref, signs_ref, out_ref,
    kv_all, packed_all, qs, acc, largest, totals, inner, rotated, weight, scales,
    local_sem, kv_send, kv_recv, kv_psend, kv_precv, p_send, p_recv, p_psend, p_precv,
    x_send, x_recv, x_psend, x_precv,
):
    rows = q_ref.shape[0]
    half_rows = rows // 2
    packed_rows = packed_ref.shape[0]
    words = packed_ref.shape[1]
    share_rows = packed_rows // share
    seg = share_rows // 2
    chips = n // 2
    kv_width = KEY_VALUE_HEADS * HEAD_SIZE

    me = lax.axis_index("blk")
    my_group = lax.axis_index("groups")
    core = lax.rem(me, 2)
    partner = me + 1 - 2 * core
    chip = me // 2
    pos = jnp.where(lax.rem(chip, 2) == 0, chip // 2, chips - 1 - chip // 2)

    def chip_at(place):
        place = lax.rem(place + chips, chips)
        return jnp.where(place < chips // 2, 2 * place, 2 * (chips - 1 - place) + 1)

    after = chip_at(pos + 1) * 2 + core
    before = chip_at(pos - 1) * 2 + core
    ring_to = (after, before)
    my_share = my_group if share > 1 else jnp.int32(0)

    barrier = pltpu.get_barrier_semaphore()
    for target in (after, before, partner):
        pl.semaphore_signal(barrier, inc=1, device_id={"blk": target}, device_id_type=MESH)
    for j in range(1, share):
        pl.semaphore_signal(
            barrier, inc=1, device_id={"groups": lax.rem(my_group + j, groups)}, device_id_type=MESH
        )
    pl.semaphore_wait(barrier, 3 + share - 1)

    def owner_chip(d, s):
        return chip_at(pos - s) if d == 0 else chip_at(pos + s)

    def kv_rows(owner, d):
        return pl.ds(pl.multiple_of(owner * rows + d * half_rows, half_rows), half_rows)

    def p_rows(owner, piece, d):
        return pl.ds(
            pl.multiple_of(owner * packed_rows + piece * share_rows + d * seg, seg), seg
        )

    def remote(src, dst, send, recv, device):
        return pltpu.make_async_remote_copy(
            src_ref=src, dst_ref=dst, send_sem=send, recv_sem=recv,
            device_id=device, device_id_type=MESH,
        )

    def kv_ring(d, s):
        where = kv_all.at[kv_rows(owner_chip(d, s) * 2 + core, d)]
        return remote(where, where, kv_send.at[d, s], kv_recv.at[d, s + 1], {"blk": ring_to[d]})

    def kv_relay(d, s):
        where = kv_all.at[kv_rows(owner_chip(d, s) * 2 + core, d)]
        return remote(where, where, kv_psend.at[d, s], kv_precv.at[d, s], {"blk": partner})

    def p_ring(d, s):
        where = packed_all.at[p_rows(owner_chip(d, s) * 2 + core, my_share, d)]
        return remote(where, where, p_send.at[d, s], p_recv.at[d, s + 1], {"blk": ring_to[d]})

    def p_relay(d, s):
        where = packed_all.at[p_rows(owner_chip(d, s) * 2 + core, my_share, d)]
        return remote(where, where, p_psend.at[d, s], p_precv.at[d, s], {"blk": partner})

    def x_copy(j, d, s):
        where = packed_all.at[p_rows(owner_chip(d, s) * 2 + core, my_share, d)]
        return remote(
            where, where, x_send.at[j - 1, d, s], x_recv.at[j - 1, d, s],
            {"groups": lax.rem(my_group + j, groups)},
        )

    def x_relay(j, d, s):
        piece = lax.rem(my_group - j + groups, groups)
        where = packed_all.at[p_rows(owner_chip(d, s) * 2 + core, piece, d)]
        return remote(
            where, where, x_psend.at[j - 1, d, s], x_precv.at[j - 1, d, s], {"blk": partner}
        )

    own_kv = kv_all.at[pl.ds(pl.multiple_of(me * rows, rows), rows)]
    own_packed = packed_all.at[pl.ds(pl.multiple_of(me * packed_rows, packed_rows), packed_rows)]
    own_rows = pl.ds(pl.multiple_of(me * rows, rows), rows)
    k_local = pltpu.make_async_copy(
        k_ref, kv_all.at[own_rows, pl.ds(0, kv_width)], local_sem.at[0]
    )
    v_local = pltpu.make_async_copy(
        v_ref, kv_all.at[own_rows, pl.ds(kv_width, kv_width)], local_sem.at[2]
    )
    p_local = pltpu.make_async_copy(packed_ref, own_packed, local_sem.at[1])
    kv_own = remote(own_kv, own_kv, kv_psend.at[0, 0], kv_precv.at[0, 0], {"blk": partner})
    p_own = remote(packed_ref, own_packed, p_psend.at[0, 0], p_precv.at[0, 0], {"blk": partner})
    k_local.start()
    v_local.start()
    p_local.start()
    k_local.wait()
    v_local.wait()
    for d in (0, 1):
        kv_ring(d, 0).start()
    kv_own.start()
    p_local.wait()
    for d in (0, 1):
        p_ring(d, 0).start()
    p_own.start()

    for h in range(QUERY_HEADS):
        g, r = divmod(h, HEAD_GROUP)
        qs[g, r * rows:(r + 1) * rows, :] = q_ref[:, h * HEAD_SIZE:(h + 1) * HEAD_SIZE]

    scales[...] = scales_ref[...].astype(jnp.float32)

    def attend(pieces, bias, first):
        tile = 2 * rows
        for g in range(KEY_VALUE_HEADS):
            k = jnp.concatenate(
                [kv_all[p, g * HEAD_SIZE:(g + 1) * HEAD_SIZE] for p in pieces], axis=0
            )
            v = jnp.concatenate(
                [kv_all[p, kv_width + g * HEAD_SIZE:kv_width + (g + 1) * HEAD_SIZE] for p in pieces],
                axis=0,
            )
            vt = v.T
            for c in range(HEAD_GROUP * rows // tile):
                cols = slice(c * tile, (c + 1) * tile)
                scores = lax.dot_general(
                    k, qs[g, cols, :], (((1,), (1,)), ((), ())), preferred_element_type=jnp.float32
                )
                scores = scores + bias
                top = jnp.max(scores, axis=0, keepdims=True)
                if not first:
                    old = largest[g, :, cols]
                    top = jnp.maximum(old, top)
                    fading = jnp.exp2((old - top) * EXPONENT)
                weights = jnp.exp2((scores - top) * EXPONENT)
                total = jnp.sum(weights, axis=0, keepdims=True)
                product = jnp.dot(
                    vt, weights.astype(jnp.bfloat16), preferred_element_type=jnp.float32
                )
                if first:
                    totals[g, :, cols] = total
                    acc[g, :, cols] = product
                else:
                    totals[g, :, cols] = totals[g, :, cols] * fading + total
                    acc[g, :, cols] = acc[g, :, cols] * fading + product
                largest[g, :, cols] = top

    chunk = math.gcd(seg, 32)

    def dequantize(row, target):
        base = packed_all[pl.ds(pl.multiple_of(row, chunk), chunk), :]
        flipped = jnp.bitwise_xor(base, jnp.int32(-2004318072))
        scale_index = row // GROUP
        for nibble in range(8):
            level = jnp.right_shift(jnp.left_shift(flipped, 28 - 4 * nibble), 28)
            scale = scales[pl.ds(scale_index, 1), nibble * words:(nibble + 1) * words]
            weight[pl.ds(pl.multiple_of(target, chunk), chunk), nibble * words:(nibble + 1) * words] = (
                level.astype(jnp.float32) * scale
            ).astype(jnp.bfloat16)

    def dequantize_rows(first_row, count):
        @pl.loop(0, count // chunk)
        def _(t):
            dequantize(first_row + t * chunk, first_row + t * chunk)

    kv_own.wait_recv()
    key_pos = chip * 2 * rows + lax.broadcasted_iota(jnp.int32, (2 * rows, 2 * rows), 0)
    query_pos = me * rows + lax.rem(lax.broadcasted_iota(jnp.int32, (2 * rows, 2 * rows), 1), rows)
    attend(
        [pl.ds(pl.multiple_of(chip * 2 * rows, 2 * rows), 2 * rows)],
        jnp.where(key_pos <= query_pos, 0.0, NEGATIVE),
        True,
    )

    def dequantize_piece(piece, s):
        @pl.loop(0, 2)
        def _(owner_core):
            for d in (0, 1):
                owner = owner_chip(d, s) * 2 + owner_core
                dequantize_rows(owner * packed_rows + piece * share_rows + d * seg, seg)

    def take_ring(s):
        for d in (0, 1):
            p_relay(d, s).wait_recv()
        if early:
            dequantize_piece(my_share, s)

    def start_relay(s):
        for d in (0, 1):
            for j in range(1, share):
                x_copy(j, d, s).wait_recv()
                x_relay(j, d, s).start()

    def take_other(s):
        for d in (0, 1):
            for j in range(1, share):
                x_relay(j, d, s).wait_recv()
        if early:
            for j in range(1, share):
                dequantize_piece(lax.rem(my_group - j + groups, groups), s)

    @pl.loop(1, chips)
    def _(s):
        for d in (0, 1):
            kv_ring(d, s - 1).wait_recv()

            @pl.when(s < chips - 1)
            def _():
                kv_ring(d, s).start()

            kv_relay(d, s).start()

        @pl.when(s == 1)
        def _():
            p_own.wait_recv()
            if early:
                dequantize_rows(chip * 2 * packed_rows, 2 * packed_rows)

        @pl.when(s > 1)
        def _():
            take_ring(s - 1)

        @pl.when(s > 2)
        def _():
            take_other(s - 2)

        for d in (0, 1):
            p_ring(d, s - 1).wait_recv()

            @pl.when(s < chips - 1)
            def _():
                p_ring(d, s).start()

            for j in range(1, share):
                x_copy(j, d, s).start()
            p_relay(d, s).start()
        for d in (0, 1):
            kv_relay(d, s).wait_recv()
        first_chip, second_chip = owner_chip(0, s), owner_chip(1, s)

        @pl.when((first_chip < chip) | (second_chip < chip))
        def _():
            key_row = lax.broadcasted_iota(jnp.int32, (2 * rows, 1), 0)
            needed = jnp.where(key_row < rows, (first_chip < chip).astype(jnp.int32), (second_chip < chip).astype(jnp.int32))
            bias = jnp.where(needed > 0, 0.0, NEGATIVE)
            attend(
                [
                    kv_rows(first_chip * 2, 0), kv_rows(first_chip * 2 + 1, 0),
                    kv_rows(second_chip * 2, 1), kv_rows(second_chip * 2 + 1, 1),
                ],
                bias, False,
            )

        @pl.when(s > 1)
        def _():
            start_relay(s - 1)

    tail = early and share > 1 and 2 * seg == HEAD_SIZE
    take_ring(chips - 1)
    if chips > 2:
        take_other(chips - 2)
    if tail:
        for owner_core in (0, 1):
            for j in range(1, share):
                piece = lax.rem(my_group - j + groups, groups)
                for d in (0, 1):
                    owner = owner_chip(d, chips - 1) * 2 + owner_core
                    weight[p_rows(owner, piece, d), :] = jnp.zeros((seg, weight.shape[1]), jnp.bfloat16)

    index = lax.broadcasted_iota(jnp.int32, (HEAD_SIZE, HEAD_SIZE), 0)
    both = jnp.bitwise_and(index, lax.broadcasted_iota(jnp.int32, (HEAD_SIZE, HEAD_SIZE), 1))
    parity = jnp.zeros_like(both)
    for bit_number in range(HEAD_SIZE.bit_length() - 1):
        parity = jnp.bitwise_xor(parity, jnp.bitwise_and(jnp.right_shift(both, bit_number), 1))
    table = (1 - 2 * parity).astype(jnp.float32).astype(jnp.bfloat16)
    for g in range(KEY_VALUE_HEADS):
        for r in range(HEAD_GROUP):
            h = g * HEAD_GROUP + r
            cols = slice(r * rows, (r + 1) * rows)
            attention = (acc[g, :, cols] / totals[g, :, cols]).T.astype(jnp.bfloat16)
            sign = (2 * signs_ref[h:h + 1, :] - 1).astype(jnp.float32).astype(jnp.bfloat16)
            signed = attention * sign
            inner[h] = jnp.dot(signed, table, preferred_element_type=jnp.float32)

    @pl.loop(0, rows // 16)
    def _(t):
        these = pl.ds(pl.multiple_of(t * 16, 16), 16)
        heads = [inner[h, these, :] for h in range(QUERY_HEADS)]
        step = 1
        while step < QUERY_HEADS:
            done = list(heads)
            for h in range(QUERY_HEADS):
                if h & step == 0:
                    done[h] = heads[h] + heads[h + step]
                    done[h + step] = heads[h] - heads[h + step]
            heads = done
            step *= 2
        for h in range(QUERY_HEADS):
            rotated[these, h * HEAD_SIZE:(h + 1) * HEAD_SIZE] = (
                heads[h] * (1.0 / math.sqrt(QUERY_HEADS * HEAD_SIZE))
            ).astype(jnp.bfloat16)

    depth = n * packed_rows
    out_width = out_ref.shape[1]
    tile = HEAD_GROUP * rows if tail else 512
    if tail:
        for c in range(out_width // tile):
            @pl.loop(0, tile // 512)
            def _(t):
                acc[c, :, pl.ds(pl.multiple_of(t * 512, 512), 512)] = jnp.dot(
                    rotated[...],
                    weight[:, pl.ds(pl.multiple_of(c * tile + t * 512, 512), 512)],
                    preferred_element_type=jnp.float32,
                )

        start_relay(chips - 1)
        take_other(chips - 1)
        lane = lax.broadcasted_iota(jnp.int32, (rows, HEAD_SIZE), 1)
        left = []
        right = []
        for owner_core in (0, 1):
            for j in range(1, share):
                piece = lax.rem(my_group - j + groups, groups)
                for d in (0, 1):
                    owner = owner_chip(d, chips - 1) * 2 + owner_core
                    begin = pl.multiple_of(owner * packed_rows + piece * share_rows, HEAD_SIZE)
                    part = rotated[:, pl.ds(begin, HEAD_SIZE)].astype(jnp.float32)
                    left.append(jnp.where(lane // seg == d, part, 0.0).astype(jnp.bfloat16))
                    right.append(pl.ds(begin, HEAD_SIZE))
        for c in range(out_width // 512):
            g, r = divmod(c * 512, tile)
            total = acc[g, :, r:r + 512]
            for part, where in zip(left, right):
                total = total + jnp.dot(
                    part, weight[where, c * 512:(c + 1) * 512], preferred_element_type=jnp.float32
                )
            out_ref[:, c * 512:(c + 1) * 512] = total.astype(jnp.bfloat16)
    else:
        start_relay(chips - 1)
        take_other(chips - 1)
    if early and not tail:
        @pl.loop(0, out_width // tile)
        def _(t):
            cols = pl.ds(pl.multiple_of(t * tile, tile), tile)
            out_ref[:, cols] = jnp.dot(
                rotated[...], weight[:, cols], preferred_element_type=jnp.float32
            ).astype(jnp.bfloat16)
    elif not early:
        span = weight.shape[0]
        tile = HEAD_GROUP * rows
        acc[...] = jnp.zeros_like(acc)

        @pl.loop(0, depth // span)
        def _(k):
            @pl.loop(0, span // chunk)
            def _(t):
                dequantize(k * span + t * chunk, t * chunk)

            left = rotated[:, pl.ds(pl.multiple_of(k * span, span), span)]
            for c in range(KEY_VALUE_HEADS):
                acc[c] += jnp.dot(
                    left, weight[:, c * tile:(c + 1) * tile], preferred_element_type=jnp.float32
                )

        for c in range(KEY_VALUE_HEADS):
            out_ref[:, c * tile:(c + 1) * tile] = acc[c].astype(jnp.bfloat16)

    kv_own.wait_send()
    p_own.wait_send()
    for d in (0, 1):
        kv_ring(d, 0).wait_send()
        p_ring(d, 0).wait_send()

    @pl.loop(1, chips)
    def _(s):
        for d in (0, 1):
            @pl.when(s < chips - 1)
            def _():
                kv_ring(d, s).wait_send()
                p_ring(d, s).wait_send()

            kv_relay(d, s).wait_send()
            p_relay(d, s).wait_send()
            for j in range(1, share):
                x_copy(j, d, s).wait_send()
                x_relay(j, d, s).wait_send()


def local(n, groups, queries, keys, values, out_packed, out_scales, hadamard_signs):
    rows = queries.shape[0]
    packed_rows, words = out_packed.shape
    width = queries.shape[1]
    share = groups if packed_rows % (32 * groups) == 0 else 1
    chips = n // 2
    kv_columns = 2 * keys.shape[1]
    signs = hadamard_signs.reshape(QUERY_HEADS, HEAD_SIZE)
    depth = n * packed_rows
    out_width = 8 * words
    kv_bytes = n * rows * kv_columns * 2
    early = kv_bytes + depth * out_width * 2 + depth * words * 4 < 46 * 2**20
    others = max(share - 1, 1)
    dma = pltpu.SemaphoreType.DMA
    spec = pl.BlockSpec(memory_space=pltpu.VMEM)
    return pl.pallas_call(
        functools.partial(kernel, n, groups, share, early),
        out_shape=jax.ShapeDtypeStruct((rows, out_width), jnp.bfloat16),
        in_specs=[spec] * 6,
        out_specs=spec,
        scratch_shapes=[
            pltpu.VMEM((n * rows, kv_columns), jnp.bfloat16),
            pltpu.VMEM((depth, words), jnp.int32),
            pltpu.VMEM((KEY_VALUE_HEADS, HEAD_GROUP * rows, HEAD_SIZE), jnp.bfloat16),
            pltpu.VMEM((KEY_VALUE_HEADS, HEAD_SIZE, HEAD_GROUP * rows), jnp.float32),
            pltpu.VMEM((KEY_VALUE_HEADS, 1, HEAD_GROUP * rows), jnp.float32),
            pltpu.VMEM((KEY_VALUE_HEADS, 1, HEAD_GROUP * rows), jnp.float32),
            pltpu.VMEM((QUERY_HEADS, rows, HEAD_SIZE), jnp.float32),
            pltpu.VMEM((rows, width), jnp.bfloat16),
            pltpu.VMEM((depth if early else 256, out_width), jnp.bfloat16),
            pltpu.VMEM(out_scales.shape, jnp.float32),
            dma((3,)),
        ]
        + [dma((2, chips))] * 8
        + [dma((others, 2, chips))] * 4,
        compiler_params=pltpu.CompilerParams(
            collective_id=0, has_side_effects=True, vmem_limit_bytes=64000000
        ),
    )(queries, keys, values, out_packed, out_scales, signs)


def solution(mesh):
    in_specs = (
        P(("groups", "blk"), None),
        P(("groups", "blk"), None),
        P(("groups", "blk"), None),
        P("blk", None),
        P(),
        P(),
    )
    out_specs = P(("groups", "blk"), None)
    body = functools.partial(local, mesh.shape["blk"], mesh.shape["groups"])
    return jax.shard_map(body, mesh=mesh, in_specs=in_specs, out_specs=out_specs, check_vma=False)
```
